32 devices in a mesh: grp: 2 (over y), seq: 4 (over z), mdl: 2 (over x), sub: 2 (over core).
Axes of the slice: x: 2, y: 2, z: 4, core: 2. Of those that a mesh axis runs over, the one named last changes fastest.
Arguments:
- frames: bfloat16 [2048, 1280], P(('grp', 'seq', 'mdl')), parts along dimension 0, may hold values from -6 to 6
- audio_count: int32 [16], P(('grp', 'seq', 'mdl')), parts along dimension 0, may hold values from 1 to 127
- pos_ids: int32 [3, 2048], P(None, ('grp', 'seq', 'mdl')), parts along dimension 1, may hold values from 0 to 4095
- gain_audio: float32 [1280], replicated, may hold values from 0.1 to 1.9
- gain_video: float32 [1280], replicated, may hold values from 0.1 to 1.9
- audio_proj: bfloat16 [1280, 3584], P(('seq', 'mdl'), 'sub'), may hold values from -0.15625 to 0.15625
- video_proj: bfloat16 [1280, 3584], P(('seq', 'mdl'), 'sub'), may hold values from -0.15625 to 0.15625
- dest_device: int32 [2048], P(('grp', 'seq', 'mdl')), parts along dimension 0, may hold values from 0 to 7, as said below
- dest_slot: int32 [2048], P(('grp', 'seq', 'mdl')), parts along dimension 0, may hold values from 0 to 127, as said below
Outputs:
- lm_rows: bfloat16 [2048, 3584], P(('grp', 'seq', 'mdl'), 'sub'), parts along dimension 0
The draws below stay inside these ranges and needn't reach their ends.
There are 2 independent parts, one for each index of `grp`. The reference program is written for one: setup_inputs(seed, part) draws one part's arguments, and reference() takes and returns one part's arrays. A program takes and returns all parts, laid end to end along the dimension named above; an argument that names none is the same for every part. Nothing has to cross between parts.
Inputs may be any that keep to these rules, and one draw needn't show every extreme that they name: The pairs (dest_device, dest_slot) name every row of the output exactly once. Each language-model shard receives exactly 128 tokens. At most 32 tokens of one source shard go to one language-model shard, and some pairs of shards reach 32. `dest_slot`: see dest_device.
All inputs are finite; a program needn't handle non-finite values.
Results may differ from the reference program's by a relative error of at most 0.0049.
Values may be sent and summed in bfloat16 or wider, within the bound.
No kernel may reach another device: no remote copies, remote signals or barrier semaphores. Data moves between devices by JAX's collectives and lax.ppermute only.
A program may use at most 64 MiB of HBM per device.

```python
import jax
import jax.numpy as jnp
from jax import lax

D_IN = 1280
D = 3584
HEAD = 128
TOK_DEV = 128
NSRC = 8
TOKENS = 1024
BLOCK = 32
N_SEQ = 4
N_MDL = 2


def routing(key):
    base = jax.random.fold_in(key, 7)
    keys = jax.random.split(base, 4)
    shard_count = N_SEQ * N_MDL
    block_count = TOK_DEV // BLOCK
    inner_order = jax.random.permutation(keys[0], shard_count).astype(jnp.int32)
    outer_order = jax.random.permutation(keys[1], shard_count).astype(jnp.int32)
    shifts = jax.random.permutation(keys[2], shard_count).astype(jnp.int32)[:block_count]
    block_order = jax.random.permutation(keys[3], block_count).astype(jnp.int32)
    everyone = jnp.arange(TOKENS, dtype=jnp.int32)
    source = everyone // TOK_DEV
    within = everyone % TOK_DEV
    block_index = within // BLOCK
    inside = within % BLOCK
    device = outer_order[(inner_order[source] + shifts[block_index]) % shard_count]
    target = block_order[block_index] * BLOCK + inside
    return (device.astype(jnp.int32), target.astype(jnp.int32))


def draw_dest_device(key, part):
    return routing(key)[0]


def draw_dest_slot(key, part):
    return routing(key)[1]


def place_ends(result, stream_key, least, top_value):
    shape = result.shape
    index_at = [jax.random.randint(jax.random.fold_in(stream_key, axis), (), 0, shape[axis]) for axis in range(len(shape))]
    result = result.at[tuple(index_at)].set(least)
    longest = shape.index(max(shape))
    index_at[longest] = (index_at[longest] + 1) % shape[longest]
    return result.at[tuple(index_at)].set(top_value)


def steps_of(stream_key, shape, pieces, least, top_value):
    def one(dim, shards_of):
        steps = jax.random.uniform(jax.random.fold_in(jax.random.fold_in(stream_key, 6), dim), (shards_of,), jnp.float32, least / len(pieces), top_value / len(pieces))
        return jnp.repeat(jnp.exp(steps), shape[dim] // shards_of).reshape((-1,) + (1,) * (len(shape) - dim - 1))

    factor_of = one(*pieces[0])
    for cut in pieces[1:]:
        factor_of = factor_of * one(*cut)
    return factor_of


def normal_values(key, extent, width, reach, shards=(), held_as=jnp.bfloat16):
    result = width * jax.random.normal(key, extent, jnp.float32)
    if shards:
        result = result * steps_of(key, extent, shards, -0.22, 0.18)
    return jnp.clip(result, -reach, reach).astype(held_as)


def setup_inputs(seed: int = 0, part: int = 0) -> dict:
    seeds = jax.random.split(jax.random.key(seed), 10)
    own_keys = jax.random.split(jax.random.fold_in(seeds[9], part), 10)
    return {
        "frames": normal_values(own_keys[0], (TOKENS, D_IN), 1.0, 6.0, ((0, 8),)),
        "audio_count": place_ends(jax.random.randint(own_keys[1], (NSRC,), 1, TOK_DEV), jax.random.fold_in(own_keys[1], 1), 1, TOK_DEV - 1).astype(jnp.int32),
        "pos_ids": place_ends(jax.random.randint(own_keys[2], (3, TOKENS), 0, 4096), jax.random.fold_in(own_keys[2], 1), 0, 4095).astype(jnp.int32),
        "gain_audio": jnp.clip(1.0 + 0.18 * jax.random.normal(seeds[3], (D_IN,), jnp.float32), 0.1, 1.9),
        "gain_video": jnp.clip(1.0 + 0.18 * jax.random.normal(seeds[4], (D_IN,), jnp.float32), 0.1, 1.9),
        "audio_proj": normal_values(seeds[5], (D_IN, D), D_IN ** -0.5, 0.15625, ((0, 8), (1, 2))),
        "video_proj": normal_values(seeds[6], (D_IN, D), D_IN ** -0.5, 0.15625, ((0, 8), (1, 2))),
        "dest_device": draw_dest_device(jax.random.fold_in(jax.random.fold_in(seeds[9], part), 71), part),
        "dest_slot": draw_dest_slot(jax.random.fold_in(jax.random.fold_in(seeds[9], part), 71), part),
    }


def normalize(frames, audio_mask, gain_audio, gain_video):
    values = frames.astype(jnp.float32)
    mean_square = lax.optimization_barrier(jnp.mean(values * values, axis=-1, keepdims=True))
    row_gain = jnp.where(audio_mask[:, None], gain_audio[None, :], gain_video[None, :])
    return (values * lax.rsqrt(mean_square + 1e-06) * row_gain).astype(jnp.bfloat16)

def rotate(values, positions):
    tok_rows = values.shape[0]
    half_size = HEAD // 2
    pair_index = jnp.arange(half_size, dtype=jnp.int32)[None, :]
    chosen = jnp.where(pair_index < HEAD // 8, positions[0][:, None], jnp.where(pair_index < HEAD * 5 // 16, positions[1][:, None], positions[2][:, None]))
    exponent = -2.0 * jnp.arange(half_size).astype(jnp.float32) / HEAD
    inverse_freq = jnp.power(jnp.float32(1000000.0), exponent)
    angles = chosen.astype(jnp.float32) * inverse_freq[None, :]
    cosine = jnp.cos(angles)[:, None, :]
    sinus = jnp.sin(angles)[:, None, :]
    by_head = values.reshape(tok_rows, -1, HEAD)
    lower = by_head[:, :, :half_size]
    second = by_head[:, :, half_size:]
    turned = jnp.concatenate([lower * cosine - second * sinus, second * cosine + lower * sinus], axis=-1)
    return turned.reshape(tok_rows, -1)

def reference(frames, audio_count, pos_ids, gain_audio, gain_video, audio_proj, video_proj, dest_device, dest_slot):
    index_local = jnp.arange(TOK_DEV, dtype=jnp.int32)

    def one_source(inputs):
        source_rows, audio_rows, positions = inputs
        audio_mask = index_local < audio_rows
        normed = normalize(source_rows, audio_mask, gain_audio, gain_video)
        from_audio = jnp.dot(normed, audio_proj, preferred_element_type=jnp.float32)
        from_video = jnp.dot(normed, video_proj, preferred_element_type=jnp.float32)
        selected = jnp.where(audio_mask[:, None], from_audio, from_video)
        return rotate(selected, positions).astype(jnp.bfloat16)
    blocks = frames.reshape(NSRC, TOK_DEV, D_IN)
    positions = pos_ids.reshape(3, NSRC, TOK_DEV).transpose(1, 0, 2)
    embedded = lax.map(one_source, (blocks, audio_count, positions)).reshape(TOKENS, D)
    target = (dest_device * TOK_DEV + dest_slot).astype(jnp.int32)
    return jnp.zeros((TOKENS, D), jnp.bfloat16).at[target].set(embedded)
```

```python
import functools

import jax
import jax.numpy as jnp
from jax import lax
from jax.experimental import pallas as pl
from jax.experimental.pallas import tpu as pltpu
from jax.sharding import PartitionSpec as P

HEAD = 128
META = 16
DIGIT = 64
F32 = jnp.float32
BF16 = jnp.bfloat16


def normalize(frames, audio_mask, gain_audio, gain_video):
    values = frames.astype(F32)
    mean_square = jnp.mean(values * values, axis=-1, keepdims=True)
    row_gain = jnp.where(audio_mask[:, None], gain_audio[None, :], gain_video[None, :])
    return (values * lax.rsqrt(mean_square + 1e-06) * row_gain).astype(BF16)


def angles_of(positions):
    half_size = HEAD // 2
    pair_index = jnp.arange(half_size, dtype=jnp.int32)[None, :]
    chosen = jnp.where(
        pair_index < HEAD // 8,
        positions[0][:, None],
        jnp.where(pair_index < HEAD * 5 // 16, positions[1][:, None], positions[2][:, None]),
    )
    exponent = -2.0 * jnp.arange(half_size).astype(F32) / HEAD
    inverse_freq = jnp.power(F32(1000000.0), exponent)
    return chosen.astype(F32) * inverse_freq[None, :]


def rotate(values, positions):
    tok_rows = values.shape[0]
    half_size = HEAD // 2
    angles = angles_of(positions)
    cosine = jnp.cos(angles)[:, None, :]
    sinus = jnp.sin(angles)[:, None, :]
    by_head = values.reshape(tok_rows, -1, HEAD)
    lower = by_head[:, :, :half_size]
    second = by_head[:, :, half_size:]
    turned = jnp.concatenate(
        [lower * cosine - second * sinus, second * cosine + lower * sinus], axis=-1
    )
    return turned.reshape(tok_rows, -1)


def gathered_plan(
    frames, audio_count, pos_ids, gain_audio, gain_video, audio_proj, video_proj, dest_device, dest_slot
):
    tok_rows = frames.shape[0]
    audio_mask = jnp.arange(tok_rows, dtype=jnp.int32) < audio_count[0]
    peer_count = lax.axis_size(("seq", "mdl"))
    capacity = 2 * tok_rows // peer_count
    onehot = (dest_device[:, None] == jnp.arange(peer_count, dtype=jnp.int32)[None, :]).astype(
        jnp.int32
    )
    arrival = jnp.sum(jnp.cumsum(onehot, axis=0) * onehot, axis=1) - 1
    bucket = dest_device * capacity + arrival
    normed = normalize(frames, audio_mask, gain_audio, gain_video)
    features = normed.shape[1]
    described = jnp.concatenate(
        [pos_ids.T, audio_mask.astype(jnp.int32)[:, None], dest_slot[:, None]], axis=1
    )
    outbox = jnp.zeros((peer_count * capacity, features), BF16).at[bucket].set(normed)
    blank_tags = jnp.concatenate(
        [
            jnp.zeros((peer_count * capacity, 4), jnp.int32),
            jnp.full((peer_count * capacity, 1), tok_rows, jnp.int32),
        ],
        axis=1,
    )
    tag_rows = blank_tags.at[bucket].set(described)
    axes = ("seq", "mdl")
    received = lax.all_to_all(outbox, axes, split_axis=0, concat_axis=0, tiled=True)
    got_tags = lax.all_to_all(tag_rows, axes, split_axis=0, concat_axis=0, tiled=True)
    arrived = got_tags[:, 4]
    placed = jnp.zeros((tok_rows, features), BF16).at[arrived].set(received, mode="drop")
    tags = jnp.zeros((tok_rows, 5), jnp.int32).at[arrived].set(got_tags, mode="drop")
    audio_full = lax.all_gather(audio_proj, axes, axis=0, tiled=True)
    video_full = lax.all_gather(video_proj, axes, axis=0, tiled=True)
    from_audio = jnp.dot(placed, audio_full, preferred_element_type=F32)
    from_video = jnp.dot(placed, video_full, preferred_element_type=F32)
    selected = jnp.where(tags[:, 3:4] > 0, from_audio, from_video)
    return rotate(selected, tags[:, :3].T).astype(BF16)


def pack_kernel(
    count_ref, frames_ref, ga_ref, gv_ref, pos_ref, dev_ref, slot_ref, *rest, zs, part
):
    outs, flipped = rest[:zs], rest[zs]
    tok_rows, features = frames_ref.shape
    z = lax.axis_index("seq")
    c = lax.axis_index("sub")
    count = count_ref[0]
    values = frames_ref[...].astype(F32)
    mean_square = jnp.mean(values * values, axis=-1, keepdims=True)
    row = lax.broadcasted_iota(jnp.int32, (tok_rows, features), 0)
    row_gain = jnp.where(row < count, ga_ref[...], gv_ref[...])
    normed = values * lax.rsqrt(mean_square + 1e-06) * row_gain
    flipped[...] = normed.T.astype(BF16)
    lane = lax.broadcasted_iota(jnp.int32, (1, tok_rows), 1)
    pos = pos_ref[...]
    facts = [dev_ref[...], slot_ref[...], (lane < count).astype(jnp.int32)]
    for k in range(3):
        facts += [pos[k : k + 1] // DIGIT, pos[k : k + 1] % DIGIT]
    line = lax.broadcasted_iota(jnp.int32, (META, tok_rows), 0)
    meta = jnp.zeros((META, tok_rows), jnp.int32)
    for k, fact in enumerate(facts):
        meta = jnp.where(line == k, fact, meta)
    meta = meta.astype(F32).astype(BF16)
    span = features // zs
    for r in range(zs):
        start = pl.multiple_of((z ^ r) * span + c * part, 16)
        outs[r][pl.ds(0, part), :] = flipped[pl.ds(start, part), :]
        outs[r][pl.ds(part, META), :] = meta


def order_kernel(mine_ref, twin_ref, oa_ref, ov_ref, pa_ref, pv_ref, meta_ref, *, zs, xs, part):
    sources, _, tok_rows = mine_ref.shape
    z = lax.axis_index("seq")
    x = lax.axis_index("mdl")
    c = lax.axis_index("sub")
    rows = zs * tok_rows
    picks = []
    for s in range(sources):
        head = mine_ref[s, pl.ds(part, META), :].astype(F32).astype(jnp.int32)
        dev, slot = head[0:1], head[1:2]
        dest_z, dest_x = dev // xs, dev % xs
        target = jnp.where(dest_x == x, (dest_z ^ z) * tok_rows + slot, -1)
        line = lax.broadcasted_iota(jnp.int32, (rows, tok_rows), 0)
        picks.append((line == target).astype(F32).astype(BF16))
    pick = jnp.concatenate(picks, axis=1)
    mine = jnp.concatenate([mine_ref[s] for s in range(sources)], axis=1)
    twin = jnp.concatenate([twin_ref[s] for s in range(sources)], axis=1)
    nt = (((1,), (1,)), ((), ()))
    got_mine = lax.dot_general(pick, mine, nt, preferred_element_type=F32)
    got_twin = lax.dot_general(pick, twin, nt, preferred_element_type=F32)
    meta_ref[...] = got_mine[:tok_rows, part:]
    audio = got_mine[:, part + 2 : part + 3] > 0.5
    same = x == c
    first = jnp.where(same, got_mine[:, :part], got_twin[:, :part])
    other = jnp.where(same, got_twin[:, :part], got_mine[:, :part])
    zero = jnp.zeros_like(first)
    oa_ref[...] = jnp.where(audio, first, zero).astype(BF16)
    ov_ref[...] = jnp.where(audio, zero, first).astype(BF16)
    pa_ref[...] = jnp.where(audio, other, zero).astype(BF16)
    pv_ref[...] = jnp.where(audio, zero, other).astype(BF16)


def project_kernel(
    oa_ref, ov_ref, pa_ref, pv_ref, own_a, own_v, peer_a, peer_v, *outs, zs, flip
):
    half = peer_a.shape[1]
    tok_rows = outs[0].shape[0]
    h = lax.axis_index("grp") ^ flip
    step = 256
    for at in range(0, half, step):
        width = min(step, half - at)
        lanes = pl.ds(pl.multiple_of(h * half + at, 128), width)
        total = jnp.dot(oa_ref[...], own_a[:, lanes], preferred_element_type=F32)
        total += jnp.dot(ov_ref[...], own_v[:, lanes], preferred_element_type=F32)
        total += jnp.dot(pa_ref[...], peer_a[:, pl.ds(at, width)], preferred_element_type=F32)
        total += jnp.dot(pv_ref[...], peer_v[:, pl.ds(at, width)], preferred_element_type=F32)
        for r in range(zs):
            block = total[r * tok_rows : (r + 1) * tok_rows]
            outs[r][:, pl.ds(at, width)] = block.astype(outs[r].dtype)


def finish_kernel(cos_ref, sin_ref, *refs, parts):
    out_ref = refs[-1]
    chunks = [refs[i * parts : (i + 1) * parts] for i in range(2)]
    half = out_ref.shape[1] // 2
    y = lax.axis_index("grp")
    cosine = jnp.concatenate([cos_ref[...], cos_ref[...]], axis=1)
    sinus = jnp.concatenate([-sin_ref[...], sin_ref[...]], axis=1)
    for flip, chunk in enumerate(chunks):
        for at in range(0, half, HEAD):
            lanes = pl.ds(at, HEAD)
            total = chunk[0][:, lanes]
            for piece in chunk[1:]:
                total = total + piece[:, lanes].astype(F32)
            turned = total * cosine + pltpu.roll(total, HEAD // 2, 1) * sinus
            where = pl.ds(pl.multiple_of((y ^ flip) * half + at, HEAD), HEAD)
            out_ref[:, where] = turned.astype(BF16)


def vmem(n):
    return [pl.BlockSpec(memory_space=pltpu.VMEM) for _ in range(n)]


def swap(value, axis, r):
    n = lax.axis_size(axis)
    return lax.ppermute(value, axis, [(i, i ^ r) for i in range(n)])


def halved_plan(
    frames, audio_count, pos_ids, gain_audio, gain_video, audio_proj, video_proj, dest_device, dest_slot
):
    tok_rows, features = frames.shape
    zs, xs = lax.axis_size("seq"), lax.axis_size("mdl")
    part = audio_proj.shape[0]
    width = audio_proj.shape[1]
    half = width // 2
    y = lax.axis_index("grp")

    near_a = swap(lax.dynamic_slice_in_dim(audio_proj, y * half, half, 1), "mdl", 1)
    near_v = swap(lax.dynamic_slice_in_dim(video_proj, y * half, half, 1), "mdl", 1)
    far_a = swap(near_a, "grp", 1)
    far_v = swap(near_v, "grp", 1)

    shape = jax.ShapeDtypeStruct
    packed = pl.pallas_call(
        functools.partial(pack_kernel, zs=zs, part=part),
        out_shape=[shape((part + META, tok_rows), BF16)] * zs,
        in_specs=[pl.BlockSpec(memory_space=pltpu.SMEM)] + vmem(6),
        out_specs=vmem(zs),
        scratch_shapes=[pltpu.VMEM((features, tok_rows), BF16)],
        name="pack",
    )(
        audio_count,
        frames,
        gain_audio[None, :],
        gain_video[None, :],
        pos_ids,
        dest_device[None, :],
        dest_slot[None, :],
    )
    column = jnp.stack([packed[0]] + [swap(packed[r], "seq", r) for r in range(zs - 1, 0, -1)])
    plane = jnp.concatenate([column, swap(column, "mdl", 1)])
    twin = swap(plane, "sub", 1)

    rows = zs * tok_rows
    *ordered, meta = pl.pallas_call(
        functools.partial(order_kernel, zs=zs, xs=xs, part=part),
        out_shape=[shape((rows, part), BF16)] * 4 + [shape((tok_rows, META), F32)],
        in_specs=vmem(2),
        out_specs=vmem(5),
        name="order",
    )(plane, twin)

    kinds = [BF16 if r % 2 else F32 for r in range(zs)]

    def project(flip, peer_a, peer_v):
        return pl.pallas_call(
            functools.partial(project_kernel, zs=zs, flip=flip),
            out_shape=[shape((tok_rows, half), kinds[r]) for r in range(zs)],
            in_specs=vmem(8),
            out_specs=vmem(zs),
            name="project",
        )(*ordered, audio_proj, video_proj, peer_a, peer_v)

    chunks = []
    for flip, (peer_a, peer_v) in enumerate([(near_a, near_v), (far_a, far_v)]):
        blocks = dict(enumerate(project(flip, peer_a, peer_v)))
        step, arrived = 1, [blocks[0]]
        while step < zs:
            later = [r for r in blocks if r % (2 * step) == step and r != step]
            moved = {r: swap(blocks[r].astype(BF16), "seq", step) for r in later}
            arrived.append(swap(blocks[step].astype(BF16), "seq", step))
            for r in later:
                blocks[r ^ step] = blocks[r ^ step].astype(F32) + moved[r].astype(F32)
            step *= 2
        chunks.append(arrived)

    whole = [meta[:, 3 + 2 * k] * DIGIT + meta[:, 4 + 2 * k] for k in range(3)]
    angles = angles_of(whole)
    return pl.pallas_call(
        functools.partial(finish_kernel, parts=len(chunks[0])),
        out_shape=shape((tok_rows, width), BF16),
        in_specs=vmem(2 + 2 * len(chunks[0])),
        out_specs=vmem(1)[0],
        name="finish",
    )(jnp.cos(angles), jnp.sin(angles), *chunks[0], *chunks[1])


def fits(mesh, features, width, tok_rows):
    size = dict(mesh.shape)
    zs = size["seq"]
    rows = features // (zs * size["mdl"])
    pairs = all(size[axis] == 2 for axis in ("grp", "mdl", "sub"))
    return pairs and zs & (zs - 1) == 0 and rows % 16 == 0 and width % 256 == 0


def solution(mesh):
    def on_device(*args):
        ok = fits(mesh, args[0].shape[1], args[5].shape[1], args[0].shape[0])
        return (halved_plan if ok else gathered_plan)(*args)

    in_specs = (
        P(("grp", "seq", "mdl"), None),
        P(("grp", "seq", "mdl")),
        P(None, ("grp", "seq", "mdl")),
        P(),
        P(),
        P(("seq", "mdl"), "sub"),
        P(("seq", "mdl"), "sub"),
        P(("grp", "seq", "mdl")),
        P(("grp", "seq", "mdl")),
    )
    out_specs = P(("grp", "seq", "mdl"), "sub")
    return jax.shard_map(
        on_device, mesh=mesh, in_specs=in_specs, out_specs=out_specs, check_vma=False
    )
```

```python
import functools
import itertools

import jax
import jax.numpy as jnp
from jax import lax
from jax.experimental import pallas as pl
from jax.experimental.pallas import tpu as pltpu
from jax.sharding import PartitionSpec as P


HEAD = 128
GRANT = 12 << 20
META = 16
DIGIT = 64
F32 = jnp.float32
BF16 = jnp.bfloat16

CUTS = (5, 2)
CHUNKS = (((0, 0),), ((0, 1), (1, 0)), ((1, 1),))


def normalize(frames, audio_mask, gain_audio, gain_video):
    values = frames.astype(F32)
    mean_square = jnp.mean(values * values, axis=-1, keepdims=True)
    row_gain = jnp.where(audio_mask[:, None], gain_audio[None, :], gain_video[None, :])
    return (values * lax.rsqrt(mean_square + 1e-06) * row_gain).astype(BF16)


def angles_of(positions):
    half_size = HEAD // 2
    pair_index = jnp.arange(half_size, dtype=jnp.int32)[None, :]
    chosen = jnp.where(
        pair_index < HEAD // 8,
        positions[0][:, None],
        jnp.where(pair_index < HEAD * 5 // 16, positions[1][:, None], positions[2][:, None]),
    )
    exponent = -2.0 * jnp.arange(half_size).astype(F32) / HEAD
    inverse_freq = jnp.power(F32(1000000.0), exponent)
    return chosen.astype(F32) * inverse_freq[None, :]


def rotate(values, positions):
    tok_rows = values.shape[0]
    half_size = HEAD // 2
    angles = angles_of(positions)
    cosine = jnp.cos(angles)[:, None, :]
    sinus = jnp.sin(angles)[:, None, :]
    by_head = values.reshape(tok_rows, -1, HEAD)
    lower = by_head[:, :, :half_size]
    second = by_head[:, :, half_size:]
    turned = jnp.concatenate(
        [lower * cosine - second * sinus, second * cosine + lower * sinus], axis=-1
    )
    return turned.reshape(tok_rows, -1)


def gathered_plan(
    frames, audio_count, pos_ids, gain_audio, gain_video, audio_proj, video_proj, dest_device, dest_slot
):
    tok_rows = frames.shape[0]
    audio_mask = jnp.arange(tok_rows, dtype=jnp.int32) < audio_count[0]
    peer_count = lax.axis_size(("seq", "mdl"))
    capacity = 2 * tok_rows // peer_count
    onehot = (dest_device[:, None] == jnp.arange(peer_count, dtype=jnp.int32)[None, :]).astype(
        jnp.int32
    )
    arrival = jnp.sum(jnp.cumsum(onehot, axis=0) * onehot, axis=1) - 1
    bucket = dest_device * capacity + arrival
    normed = normalize(frames, audio_mask, gain_audio, gain_video)
    features = normed.shape[1]
    described = jnp.concatenate(
        [pos_ids.T, audio_mask.astype(jnp.int32)[:, None], dest_slot[:, None]], axis=1
    )
    outbox = jnp.zeros((peer_count * capacity, features), BF16).at[bucket].set(normed)
    blank_tags = jnp.concatenate(
        [
            jnp.zeros((peer_count * capacity, 4), jnp.int32),
            jnp.full((peer_count * capacity, 1), tok_rows, jnp.int32),
        ],
        axis=1,
    )
    tag_rows = blank_tags.at[bucket].set(described)
    axes = ("seq", "mdl")
    received = lax.all_to_all(outbox, axes, split_axis=0, concat_axis=0, tiled=True)
    got_tags = lax.all_to_all(tag_rows, axes, split_axis=0, concat_axis=0, tiled=True)
    arrived = got_tags[:, 4]
    placed = jnp.zeros((tok_rows, features), BF16).at[arrived].set(received, mode="drop")
    tags = jnp.zeros((tok_rows, 5), jnp.int32).at[arrived].set(got_tags, mode="drop")
    audio_full = lax.all_gather(audio_proj, axes, axis=0, tiled=True)
    video_full = lax.all_gather(video_proj, axes, axis=0, tiled=True)
    from_audio = jnp.dot(placed, audio_full, preferred_element_type=F32)
    from_video = jnp.dot(placed, video_full, preferred_element_type=F32)
    selected = jnp.where(tags[:, 3:4] > 0, from_audio, from_video)
    return rotate(selected, tags[:, :3].T).astype(BF16)


def pack_kernel(count_ref, *refs, zs, part):
    given, outs, held = refs[:6], refs[6 : 6 + zs], refs[6 + zs : 12 + zs]
    flipped, arrived = refs[12 + zs :]
    loads = [pltpu.make_async_copy(a, b, arrived.at[i]) for i, (a, b) in enumerate(zip(given, held))]
    for load in loads:
        load.start()
    frames_ref, ga_ref, gv_ref, pos_ref, dev_ref, slot_ref = held
    tok_rows, features = frames_ref.shape
    z = lax.axis_index("seq")
    c = lax.axis_index("sub")
    count = count_ref[0]
    for load in loads:
        load.wait()
    values = frames_ref[...].astype(F32)
    mean_square = jnp.mean(values * values, axis=-1, keepdims=True)
    row = lax.broadcasted_iota(jnp.int32, (tok_rows, features), 0)
    row_gain = jnp.where(row < count, ga_ref[...][None, :], gv_ref[...][None, :])
    normed = values * lax.rsqrt(mean_square + 1e-06) * row_gain
    flipped[...] = normed.T.astype(BF16)
    lane = lax.broadcasted_iota(jnp.int32, (1, tok_rows), 1)
    pos = pos_ref[...]
    facts = [dev_ref[...][None, :], slot_ref[...][None, :], (lane < count).astype(jnp.int32)]
    for k in range(3):
        facts += [pos[k : k + 1] // DIGIT, pos[k : k + 1] % DIGIT]
    line = lax.broadcasted_iota(jnp.int32, (META, tok_rows), 0)
    meta = jnp.zeros((META, tok_rows), jnp.int32)
    for k, fact in enumerate(facts):
        meta = jnp.where(line == k, fact, meta)
    meta = meta.astype(F32).astype(BF16)
    span = features // zs
    for r in range(zs):
        start = pl.multiple_of((z ^ r) * span + c * part, 16)
        outs[r][pl.ds(0, part), :] = flipped[pl.ds(start, part), :]
        outs[r][pl.ds(part, META), :] = meta


def order_kernel(*refs, zs, xs, part, rels):
    own_refs, twin_refs, outs = refs[:2], refs[2:4], refs[4:]
    tok_rows = own_refs[0].shape[2]
    z = lax.axis_index("seq")
    x = lax.axis_index("mdl")
    c = lax.axis_index("sub")
    rows = len(rels) * tok_rows
    picks = []
    for ref in own_refs:
        for s in range(zs):
            head = ref[s, pl.ds(part, META), :].astype(F32).astype(jnp.int32)
            dev, slot = head[0:1], head[1:2]
            rel = (dev // xs) ^ z
            target = jnp.full_like(rel, -1)
            for i, r in enumerate(rels):
                target = jnp.where(rel == r, i * tok_rows + slot, target)
            target = jnp.where(dev % xs == x, target, -1)
            line = lax.broadcasted_iota(jnp.int32, (rows, tok_rows), 0)
            picks.append((line == target).astype(F32).astype(BF16))
    pick = jnp.concatenate(picks, axis=1)
    nt = (((1,), (1,)), ((), ()))
    got = []
    for side in (own_refs, twin_refs):
        wide = jnp.concatenate([ref[s] for ref in side for s in range(zs)], axis=1)
        got.append(lax.dot_general(pick, wide, nt, preferred_element_type=F32))
    if rels[0] == 0:
        outs[4][...] = got[0][:tok_rows, part:]
    audio = got[0][:, part + 2 : part + 3] > 0.5
    same = x == c
    first = jnp.where(same, got[0][:, :part], got[1][:, :part])
    other = jnp.where(same, got[1][:, :part], got[0][:, :part])
    for k, values in enumerate((first, other)):
        outs[2 * k][...] = jnp.where(audio, values, 0.0).astype(BF16)
        outs[2 * k + 1][...] = jnp.where(audio, 0.0, values).astype(BF16)


def project_kernel(oa_ref, ov_ref, pa_ref, pv_ref, own_a, own_v, *refs, places):
    peers, outs = refs[: len(places)], refs[len(places) :]
    part, half = own_a.shape[0], own_a.shape[1] // 2
    tok_rows = outs[0].shape[0]
    step = 256
    done = 0
    for (flip, base), peer_ref in zip(places, peers):
        h = lax.axis_index("grp") ^ flip
        for at in range(0, peer_ref.shape[1], step):
            size = min(step, peer_ref.shape[1] - at)
            lanes = pl.ds(pl.multiple_of(h * half + base + at, 128), size)
            there = pl.ds(at, size)
            total = jnp.dot(oa_ref[...], own_a[:, lanes], preferred_element_type=F32)
            total += jnp.dot(ov_ref[...], own_v[:, lanes], preferred_element_type=F32)
            total += jnp.dot(pa_ref[...], peer_ref[:part, there], preferred_element_type=F32)
            total += jnp.dot(pv_ref[...], peer_ref[part:, there], preferred_element_type=F32)
            for i, out in enumerate(outs):
                block = total[i * tok_rows : (i + 1) * tok_rows]
                out[:, pl.ds(done + at, size)] = block.astype(out.dtype)
        done += peer_ref.shape[1]


def finish_kernel(cos_ref, sin_ref, *refs, places):
    out_ref = refs[-1]
    parts = (len(refs) - 1) // len(places)
    half = out_ref.shape[1] // 2
    y = lax.axis_index("grp")
    cosine = jnp.concatenate([cos_ref[...], cos_ref[...]], axis=1)
    sinus = jnp.concatenate([-sin_ref[...], sin_ref[...]], axis=1)
    for i, pieces in enumerate(places):
        chunk = refs[i * parts : (i + 1) * parts]
        at = 0
        for flip, base, size in pieces:
            for head in range(0, size, HEAD):
                lanes = pl.ds(at, HEAD)
                total = chunk[0][:, lanes]
                for piece in chunk[1:]:
                    total = total + piece[:, lanes].astype(F32)
                turned = total * cosine + pltpu.roll(total, HEAD // 2, 1) * sinus
                where = pl.ds(pl.multiple_of((y ^ flip) * half + base + head, HEAD), HEAD)
                out_ref[:, where] = turned.astype(BF16)
                at += HEAD


def vmem(n):
    return [pl.BlockSpec(memory_space=pltpu.VMEM) for _ in range(n)]


def swap(value, axis, r):
    n = lax.axis_size(axis)
    return lax.ppermute(value, axis, [(i, i ^ r) for i in range(n)])


def halved_plan(
    frames, audio_count, pos_ids, gain_audio, gain_video, audio_proj, video_proj, dest_device, dest_slot
):
    tok_rows, features = frames.shape
    zs, xs = lax.axis_size("seq"), lax.axis_size("mdl")
    part = audio_proj.shape[0]
    width = audio_proj.shape[1]
    half = width // 2
    y = lax.axis_index("grp")

    heads = half // HEAD
    marks = [heads * at // sum(CUTS) * HEAD for at in itertools.accumulate(CUTS, initial=0)]
    cuts = [(a, b - a) for a, b in zip(marks, marks[1:])]
    row, rest = [], []
    for i, (base, size) in enumerate(cuts):
        both = [
            lax.dynamic_slice_in_dim(proj, y * half + base, size, 1)
            for proj in (audio_proj, video_proj)
        ]
        row.append(swap(jnp.concatenate(both), "mdl", 1))
        rest.append(swap(row[i], "grp", 1))

    shape = jax.ShapeDtypeStruct
    given = (frames, gain_audio, gain_video, pos_ids, dest_device, dest_slot)
    packed = pl.pallas_call(
        functools.partial(pack_kernel, zs=zs, part=part),
        out_shape=[shape((part + META, tok_rows), BF16)] * zs,
        in_specs=[pl.BlockSpec(memory_space=pltpu.SMEM)]
        + [pl.BlockSpec(memory_space=pltpu.HBM) for _ in given],
        out_specs=vmem(zs),
        scratch_shapes=[pltpu.VMEM(a.shape, a.dtype) for a in given]
        + [pltpu.VMEM((features, tok_rows), BF16), pltpu.SemaphoreType.DMA((len(given),))],
        compiler_params=pltpu.CompilerParams(vmem_limit_bytes=GRANT),
        name="pack",
    )(audio_count, *given)
    column = jnp.stack([packed[0]] + [swap(packed[r], "seq", r) for r in range(zs - 1, 0, -1)])
    crossed = swap(column, "mdl", 1)
    twins = [swap(v, "sub", 1) for v in (column, crossed)]

    ahead = [r for r in range(zs) if r % 2 and r > 1]
    groups = [ahead, [r for r in range(zs) if r not in ahead]]
    ordered = []
    for rels in groups:
        extra = [shape((tok_rows, META), F32)] if rels[0] == 0 else []
        call = pl.pallas_call(
            functools.partial(order_kernel, zs=zs, xs=xs, part=part, rels=rels),
            out_shape=[shape((len(rels) * tok_rows, part), BF16)] * 4 + extra,
            in_specs=vmem(4),
            out_specs=vmem(4 + len(extra)),
            compiler_params=pltpu.CompilerParams(vmem_limit_bytes=GRANT),
            name="order",
        )
        ordered.append(call(column, crossed, *twins))
    meta = ordered[1][4]

    def project(pieces):
        peers = [(rest if flip else row)[i] for i, flip in pieces]
        across = sum(peer.shape[1] for peer in peers)
        at = tuple((flip, cuts[i][0]) for i, flip in pieces)
        blocks = {}
        for g, rels in enumerate(groups):
            call = pl.pallas_call(
                functools.partial(project_kernel, places=at),
                out_shape=[shape((tok_rows, across), BF16 if r % 2 else F32) for r in rels],
                in_specs=vmem(6 + len(peers)),
                out_specs=vmem(len(rels)),
                compiler_params=pltpu.CompilerParams(vmem_limit_bytes=GRANT),
                name="project",
            )
            made = call(*ordered[g][:4], audio_proj, video_proj, *peers)
            blocks.update(zip(rels, made))
        return blocks

    chunks, places = [], []
    for pieces in CHUNKS:
        blocks = project(pieces)
        step, arrived = 1, [blocks[0]]
        while step < zs:
            later = [r for r in blocks if r % (2 * step) == step and r != step]
            moved = {r: swap(blocks[r].astype(BF16), "seq", step) for r in later}
            arrived.append(swap(blocks[step].astype(BF16), "seq", step))
            for r in later:
                blocks[r ^ step] = blocks[r ^ step].astype(F32) + moved[r].astype(F32)
            step *= 2
        chunks += arrived
        places.append(tuple((flip, *cuts[i]) for i, flip in pieces))

    whole = [meta[:, 3 + 2 * k] * DIGIT + meta[:, 4 + 2 * k] for k in range(3)]
    angles = angles_of(whole)
    return pl.pallas_call(
        functools.partial(finish_kernel, places=places),
        out_shape=shape((tok_rows, width), BF16),
        in_specs=vmem(2 + len(chunks)),
        out_specs=vmem(1)[0],
        compiler_params=pltpu.CompilerParams(vmem_limit_bytes=GRANT),
        name="finish",
    )(jnp.cos(angles), jnp.sin(angles), *chunks)


def fits(mesh, features, width):
    size = dict(mesh.shape)
    zs = size["seq"]
    rows = features // (zs * size["mdl"])
    pairs = all(size[axis] == 2 for axis in ("grp", "mdl", "sub"))
    return pairs and zs > 2 and zs & (zs - 1) == 0 and rows % 16 == 0 and width % 256 == 0


def solution(mesh):
    def on_device(*args):
        ok = fits(mesh, args[0].shape[1], args[5].shape[1])
        return (halved_plan if ok else gathered_plan)(*args)

    in_specs = (
        P(("grp", "seq", "mdl"), None),
        P(("grp", "seq", "mdl")),
        P(None, ("grp", "seq", "mdl")),
        P(),
        P(),
        P(("seq", "mdl"), "sub"),
        P(("seq", "mdl"), "sub"),
        P(("grp", "seq", "mdl")),
        P(("grp", "seq", "mdl")),
    )
    out_specs = P(("grp", "seq", "mdl"), "sub")
    return jax.shard_map(
        on_device, mesh=mesh, in_specs=in_specs, out_specs=out_specs, check_vma=False
    )
```

```python
import functools
import itertools

import jax
import jax.numpy as jnp
from jax import lax
from jax.experimental import pallas as pl
from jax.experimental.pallas import tpu as pltpu
from jax.sharding import PartitionSpec as P


HEAD = 128
GRANT = 12 << 20
META = 16
DIGIT = 64
F32 = jnp.float32
BF16 = jnp.bfloat16

CUTS = (4, 3)
CHUNKS = (((0, 0),), ((0, 1), (1, 0)), ((1, 1),))


def normalize(frames, audio_mask, gain_audio, gain_video):
    values = frames.astype(F32)
    mean_square = jnp.mean(values * values, axis=-1, keepdims=True)
    row_gain = jnp.where(audio_mask[:, None], gain_audio[None, :], gain_video[None, :])
    return (values * lax.rsqrt(mean_square + 1e-06) * row_gain).astype(BF16)


def angles_of(positions):
    half_size = HEAD // 2
    pair_index = jnp.arange(half_size, dtype=jnp.int32)[None, :]
    chosen = jnp.where(
        pair_index < HEAD // 8,
        positions[0][:, None],
        jnp.where(pair_index < HEAD * 5 // 16, positions[1][:, None], positions[2][:, None]),
    )
    exponent = -2.0 * jnp.arange(half_size).astype(F32) / HEAD
    inverse_freq = jnp.power(F32(1000000.0), exponent)
    return chosen.astype(F32) * inverse_freq[None, :]


def rotate(values, positions):
    tok_rows = values.shape[0]
    half_size = HEAD // 2
    angles = angles_of(positions)
    cosine = jnp.cos(angles)[:, None, :]
    sinus = jnp.sin(angles)[:, None, :]
    by_head = values.reshape(tok_rows, -1, HEAD)
    lower = by_head[:, :, :half_size]
    second = by_head[:, :, half_size:]
    turned = jnp.concatenate(
        [lower * cosine - second * sinus, second * cosine + lower * sinus], axis=-1
    )
    return turned.reshape(tok_rows, -1)


def gathered_plan(
    frames, audio_count, pos_ids, gain_audio, gain_video, audio_proj, video_proj, dest_device, dest_slot
):
    tok_rows = frames.shape[0]
    audio_mask = jnp.arange(tok_rows, dtype=jnp.int32) < audio_count[0]
    peer_count = lax.axis_size(("seq", "mdl"))
    capacity = 2 * tok_rows // peer_count
    onehot = (dest_device[:, None] == jnp.arange(peer_count, dtype=jnp.int32)[None, :]).astype(
        jnp.int32
    )
    arrival = jnp.sum(jnp.cumsum(onehot, axis=0) * onehot, axis=1) - 1
    bucket = dest_device * capacity + arrival
    normed = normalize(frames, audio_mask, gain_audio, gain_video)
    features = normed.shape[1]
    described = jnp.concatenate(
        [pos_ids.T, audio_mask.astype(jnp.int32)[:, None], dest_slot[:, None]], axis=1
    )
    outbox = jnp.zeros((peer_count * capacity, features), BF16).at[bucket].set(normed)
    blank_tags = jnp.concatenate(
        [
            jnp.zeros((peer_count * capacity, 4), jnp.int32),
            jnp.full((peer_count * capacity, 1), tok_rows, jnp.int32),
        ],
        axis=1,
    )
    tag_rows = blank_tags.at[bucket].set(described)
    axes = ("seq", "mdl")
    received = lax.all_to_all(outbox, axes, split_axis=0, concat_axis=0, tiled=True)
    got_tags = lax.all_to_all(tag_rows, axes, split_axis=0, concat_axis=0, tiled=True)
    arrived = got_tags[:, 4]
    placed = jnp.zeros((tok_rows, features), BF16).at[arrived].set(received, mode="drop")
    tags = jnp.zeros((tok_rows, 5), jnp.int32).at[arrived].set(got_tags, mode="drop")
    audio_full = lax.all_gather(audio_proj, axes, axis=0, tiled=True)
    video_full = lax.all_gather(video_proj, axes, axis=0, tiled=True)
    from_audio = jnp.dot(placed, audio_full, preferred_element_type=F32)
    from_video = jnp.dot(placed, video_full, preferred_element_type=F32)
    selected = jnp.where(tags[:, 3:4] > 0, from_audio, from_video)
    return rotate(selected, tags[:, :3].T).astype(BF16)


def pack_kernel(
    frames_ref, ga_ref, gv_ref, pos_ref, dev_ref, slot_ref, count_ref, *rest, zs, part
):
    outs, flipped = rest[:zs], rest[zs]
    tok_rows, features = frames_ref.shape
    z = lax.axis_index("seq")
    c = lax.axis_index("sub")
    count = count_ref[...][None, :]
    values = frames_ref[...].astype(F32)
    mean_square = jnp.mean(values * values, axis=-1, keepdims=True)
    row = lax.broadcasted_iota(jnp.int32, (tok_rows, features), 0)
    row_gain = jnp.where(row < count, ga_ref[...][None, :], gv_ref[...][None, :])
    normed = values * lax.rsqrt(mean_square + 1e-06) * row_gain
    flipped[...] = normed.T.astype(BF16)
    lane = lax.broadcasted_iota(jnp.int32, (1, tok_rows), 1)
    pos = pos_ref[...]
    facts = [dev_ref[...][None, :], slot_ref[...][None, :], (lane < count).astype(jnp.int32)]
    for k in range(3):
        facts += [pos[k : k + 1] // DIGIT, pos[k : k + 1] % DIGIT]
    line = lax.broadcasted_iota(jnp.int32, (META, tok_rows), 0)
    meta = jnp.zeros((META, tok_rows), jnp.int32)
    for k, fact in enumerate(facts):
        meta = jnp.where(line == k, fact, meta)
    meta = meta.astype(F32).astype(BF16)
    span = features // zs
    for r in range(zs):
        start = pl.multiple_of((z ^ r) * span + c * part, 16)
        outs[r][pl.ds(0, part), :] = flipped[pl.ds(start, part), :]
        outs[r][pl.ds(part, META), :] = meta


def order_kernel(*refs, zs, xs, part, rels):
    own_refs, twin_refs, outs = refs[:2], refs[2:4], refs[4:]
    tok_rows = own_refs[0].shape[2]
    z = lax.axis_index("seq")
    x = lax.axis_index("mdl")
    c = lax.axis_index("sub")
    rows = len(rels) * tok_rows
    picks = []
    for ref in own_refs:
        for s in range(zs):
            head = ref[s, pl.ds(part, META), :].astype(F32).astype(jnp.int32)
            dev, slot = head[0:1], head[1:2]
            rel = (dev // xs) ^ z
            target = jnp.full_like(rel, -1)
            for i, r in enumerate(rels):
                target = jnp.where(rel == r, i * tok_rows + slot, target)
            target = jnp.where(dev % xs == x, target, -1)
            line = lax.broadcasted_iota(jnp.int32, (rows, tok_rows), 0)
            picks.append((line == target).astype(F32).astype(BF16))
    pick = jnp.concatenate(picks, axis=1)
    nt = (((1,), (1,)), ((), ()))
    got = []
    for side in (own_refs, twin_refs):
        wide = jnp.concatenate([ref[s] for ref in side for s in range(zs)], axis=1)
        got.append(lax.dot_general(pick, wide, nt, preferred_element_type=F32))
    if rels[0] == 0:
        outs[4][...] = got[0][:tok_rows, part:]
    audio = got[0][:, part + 2 : part + 3] > 0.5
    same = x == c
    first = jnp.where(same, got[0][:, :part], got[1][:, :part])
    other = jnp.where(same, got[1][:, :part], got[0][:, :part])
    for k, values in enumerate((first, other)):
        outs[2 * k][...] = jnp.where(audio, values, 0.0).astype(BF16)
        outs[2 * k + 1][...] = jnp.where(audio, 0.0, values).astype(BF16)


def project_kernel(oa_ref, ov_ref, pa_ref, pv_ref, own_a, own_v, *refs, places):
    peers, outs = refs[: len(places)], refs[len(places) :]
    part, half = own_a.shape[0], own_a.shape[1] // 2
    tok_rows = outs[0].shape[0]
    step = 256
    done = 0
    for (flip, base), peer_ref in zip(places, peers):
        h = lax.axis_index("grp") ^ flip
        for at in range(0, peer_ref.shape[1], step):
            size = min(step, peer_ref.shape[1] - at)
            lanes = pl.ds(pl.multiple_of(h * half + base + at, 128), size)
            there = pl.ds(at, size)
            total = jnp.dot(oa_ref[...], own_a[:, lanes], preferred_element_type=F32)
            total += jnp.dot(ov_ref[...], own_v[:, lanes], preferred_element_type=F32)
            total += jnp.dot(pa_ref[...], peer_ref[:part, there], preferred_element_type=F32)
            total += jnp.dot(pv_ref[...], peer_ref[part:, there], preferred_element_type=F32)
            for i, out in enumerate(outs):
                block = total[i * tok_rows : (i + 1) * tok_rows]
                out[:, pl.ds(done + at, size)] = block.astype(out.dtype)
        done += peer_ref.shape[1]


def finish_kernel(cos_ref, sin_ref, *refs, places):
    out_ref, turned_ref, sent = refs[-3:]
    parts = len(refs[:-3]) // len(places)
    half = out_ref.shape[1] // 2
    y = lax.axis_index("grp")
    cosine = jnp.concatenate([cos_ref[...], cos_ref[...]], axis=1)
    sinus = jnp.concatenate([-sin_ref[...], sin_ref[...]], axis=1)
    copies, begin = [], 0
    for i, pieces in enumerate(places):
        chunk = refs[i * parts : (i + 1) * parts]
        at = 0
        for flip, base, size in pieces:
            for head in range(0, size, HEAD):
                lanes = pl.ds(at + head, HEAD)
                total = chunk[0][:, lanes]
                for piece in chunk[1:]:
                    total = total + piece[:, lanes].astype(F32)
                turned = total * cosine + pltpu.roll(total, HEAD // 2, 1) * sinus
                turned_ref[:, pl.ds(begin + head, HEAD)] = turned.astype(BF16)
            where = pl.ds(pl.multiple_of((y ^ flip) * half + base, HEAD), size)
            source = turned_ref.at[:, pl.ds(begin, size)]
            copies.append(
                pltpu.make_async_copy(source, out_ref.at[:, where], sent.at[len(copies)])
            )
            copies[-1].start()
            at, begin = at + size, begin + size
    for copy in copies:
        copy.wait()


def vmem(n):
    return [pl.BlockSpec(memory_space=pltpu.VMEM) for _ in range(n)]


def swap(value, axis, r):
    n = lax.axis_size(axis)
    return lax.ppermute(value, axis, [(i, i ^ r) for i in range(n)])


def halved_plan(
    frames, audio_count, pos_ids, gain_audio, gain_video, audio_proj, video_proj, dest_device, dest_slot
):
    tok_rows, features = frames.shape
    zs, xs = lax.axis_size("seq"), lax.axis_size("mdl")
    part = audio_proj.shape[0]
    width = audio_proj.shape[1]
    half = width // 2
    y = lax.axis_index("grp")

    heads = half // HEAD
    marks = [heads * at // sum(CUTS) * HEAD for at in itertools.accumulate(CUTS, initial=0)]
    cuts = [(a, b - a) for a, b in zip(marks, marks[1:])]
    row, rest = [], []
    for i, (base, size) in enumerate(cuts):
        both = [
            lax.dynamic_slice_in_dim(proj, y * half + base, size, 1)
            for proj in (audio_proj, video_proj)
        ]
        row.append(swap(jnp.concatenate(both), "mdl", 1))
        rest.append(swap(row[i], "grp", 1))

    shape = jax.ShapeDtypeStruct
    given = (frames, gain_audio, gain_video, pos_ids, dest_device, dest_slot, audio_count)
    packed = pl.pallas_call(
        functools.partial(pack_kernel, zs=zs, part=part),
        out_shape=[shape((part + META, tok_rows), BF16)] * zs,
        in_specs=vmem(len(given)),
        out_specs=vmem(zs),
        scratch_shapes=[pltpu.VMEM((features, tok_rows), BF16)],
        compiler_params=pltpu.CompilerParams(vmem_limit_bytes=GRANT),
        name="pack",
    )(*given)
    column = jnp.stack([packed[0]] + [swap(packed[r], "seq", r) for r in range(zs - 1, 0, -1)])
    crossed = swap(column, "mdl", 1)
    twins = [swap(v, "sub", 1) for v in (column, crossed)]

    ahead = [r for r in range(zs) if r % 2 and r > 1]
    groups = [ahead, [r for r in range(zs) if r not in ahead]]
    ordered = []
    for rels in groups:
        extra = [shape((tok_rows, META), F32)] if rels[0] == 0 else []
        call = pl.pallas_call(
            functools.partial(order_kernel, zs=zs, xs=xs, part=part, rels=rels),
            out_shape=[shape((len(rels) * tok_rows, part), BF16)] * 4 + extra,
            in_specs=vmem(4),
            out_specs=vmem(4 + len(extra)),
            compiler_params=pltpu.CompilerParams(vmem_limit_bytes=GRANT),
            name="order",
        )
        ordered.append(call(column, crossed, *twins))
    meta = ordered[1][4]

    def project(pieces):
        peers = [(rest if flip else row)[i] for i, flip in pieces]
        across = sum(peer.shape[1] for peer in peers)
        at = tuple((flip, cuts[i][0]) for i, flip in pieces)
        blocks = {}
        for g, rels in enumerate(groups):
            call = pl.pallas_call(
                functools.partial(project_kernel, places=at),
                out_shape=[shape((tok_rows, across), BF16 if r % 2 else F32) for r in rels],
                in_specs=vmem(6 + len(peers)),
                out_specs=vmem(len(rels)),
                compiler_params=pltpu.CompilerParams(vmem_limit_bytes=GRANT),
                name="project",
            )
            made = call(*ordered[g][:4], audio_proj, video_proj, *peers)
            blocks.update(zip(rels, made))
        return blocks

    chunks, places = [], []
    for pieces in CHUNKS:
        blocks = project(pieces)
        step, arrived = 1, [blocks[0]]
        while step < zs:
            later = [r for r in blocks if r % (2 * step) == step and r != step]
            moved = {r: swap(blocks[r].astype(BF16), "seq", step) for r in later}
            arrived.append(swap(blocks[step].astype(BF16), "seq", step))
            for r in later:
                blocks[r ^ step] = blocks[r ^ step].astype(F32) + moved[r].astype(F32)
            step *= 2
        chunks += arrived
        places.append(tuple((flip, *cuts[i]) for i, flip in pieces))

    whole = [meta[:, 3 + 2 * k] * DIGIT + meta[:, 4 + 2 * k] for k in range(3)]
    angles = angles_of(whole)
    return pl.pallas_call(
        functools.partial(finish_kernel, places=places),
        out_shape=shape((tok_rows, width), BF16),
        in_specs=vmem(2 + len(chunks)),
        out_specs=pl.BlockSpec(memory_space=pltpu.HBM),
        scratch_shapes=[
            pltpu.VMEM((tok_rows, width), BF16),
            pltpu.SemaphoreType.DMA((sum(len(place) for place in places),)),
        ],
        compiler_params=pltpu.CompilerParams(vmem_limit_bytes=GRANT),
        name="finish",
    )(jnp.cos(angles), jnp.sin(angles), *chunks)


def fits(mesh, features, width):
    size = dict(mesh.shape)
    zs = size["seq"]
    rows = features // (zs * size["mdl"])
    pairs = all(size[axis] == 2 for axis in ("grp", "mdl", "sub"))
    return pairs and zs > 2 and zs & (zs - 1) == 0 and rows % 16 == 0 and width % 256 == 0


def solution(mesh):
    def on_device(*args):
        ok = fits(mesh, args[0].shape[1], args[5].shape[1])
        return (halved_plan if ok else gathered_plan)(*args)

    in_specs = (
        P(("grp", "seq", "mdl"), None),
        P(("grp", "seq", "mdl")),
        P(None, ("grp", "seq", "mdl")),
        P(),
        P(),
        P(("seq", "mdl"), "sub"),
        P(("seq", "mdl"), "sub"),
        P(("grp", "seq", "mdl")),
        P(("grp", "seq", "mdl")),
    )
    out_specs = P(("grp", "seq", "mdl"), "sub")
    return jax.shard_map(
        on_device, mesh=mesh, in_specs=in_specs, out_specs=out_specs, check_vma=False
    )
```

```python
import functools
import itertools

import jax
import jax.numpy as jnp
from jax import lax
from jax.experimental import pallas as pl
from jax.experimental.pallas import tpu as pltpu
from jax.sharding import PartitionSpec as P


HEAD = 128
GRANT = 12 << 20
META = 16
DIGIT = 64
F32 = jnp.float32
BF16 = jnp.bfloat16

CUTS = (4, 3)
CHUNKS = (((0, 0),), ((0, 1), (1, 0)), ((1, 1),))

ARRIVAL = (2, 3, 1)


def normalize(frames, audio_mask, gain_audio, gain_video):
    values = frames.astype(F32)
    mean_square = jnp.mean(values * values, axis=-1, keepdims=True)
    row_gain = jnp.where(audio_mask[:, None], gain_audio[None, :], gain_video[None, :])
    return (values * lax.rsqrt(mean_square + 1e-06) * row_gain).astype(BF16)


def angles_of(positions):
    half_size = HEAD // 2
    pair_index = jnp.arange(half_size, dtype=jnp.int32)[None, :]
    chosen = jnp.where(
        pair_index < HEAD // 8,
        positions[0][:, None],
        jnp.where(pair_index < HEAD * 5 // 16, positions[1][:, None], positions[2][:, None]),
    )
    exponent = -2.0 * jnp.arange(half_size).astype(F32) / HEAD
    inverse_freq = jnp.power(F32(1000000.0), exponent)
    return chosen.astype(F32) * inverse_freq[None, :]


def rotate(values, positions):
    tok_rows = values.shape[0]
    half_size = HEAD // 2
    angles = angles_of(positions)
    cosine = jnp.cos(angles)[:, None, :]
    sinus = jnp.sin(angles)[:, None, :]
    by_head = values.reshape(tok_rows, -1, HEAD)
    lower = by_head[:, :, :half_size]
    second = by_head[:, :, half_size:]
    turned = jnp.concatenate(
        [lower * cosine - second * sinus, second * cosine + lower * sinus], axis=-1
    )
    return turned.reshape(tok_rows, -1)


def gathered_plan(
    frames, audio_count, pos_ids, gain_audio, gain_video, audio_proj, video_proj, dest_device, dest_slot
):
    tok_rows = frames.shape[0]
    audio_mask = jnp.arange(tok_rows, dtype=jnp.int32) < audio_count[0]
    peer_count = lax.axis_size(("seq", "mdl"))
    capacity = 2 * tok_rows // peer_count
    onehot = (dest_device[:, None] == jnp.arange(peer_count, dtype=jnp.int32)[None, :]).astype(
        jnp.int32
    )
    arrival = jnp.sum(jnp.cumsum(onehot, axis=0) * onehot, axis=1) - 1
    bucket = dest_device * capacity + arrival
    normed = normalize(frames, audio_mask, gain_audio, gain_video)
    features = normed.shape[1]
    described = jnp.concatenate(
        [pos_ids.T, audio_mask.astype(jnp.int32)[:, None], dest_slot[:, None]], axis=1
    )
    outbox = jnp.zeros((peer_count * capacity, features), BF16).at[bucket].set(normed)
    blank_tags = jnp.concatenate(
        [
            jnp.zeros((peer_count * capacity, 4), jnp.int32),
            jnp.full((peer_count * capacity, 1), tok_rows, jnp.int32),
        ],
        axis=1,
    )
    tag_rows = blank_tags.at[bucket].set(described)
    axes = ("seq", "mdl")
    received = lax.all_to_all(outbox, axes, split_axis=0, concat_axis=0, tiled=True)
    got_tags = lax.all_to_all(tag_rows, axes, split_axis=0, concat_axis=0, tiled=True)
    arrived = got_tags[:, 4]
    placed = jnp.zeros((tok_rows, features), BF16).at[arrived].set(received, mode="drop")
    tags = jnp.zeros((tok_rows, 5), jnp.int32).at[arrived].set(got_tags, mode="drop")
    audio_full = lax.all_gather(audio_proj, axes, axis=0, tiled=True)
    video_full = lax.all_gather(video_proj, axes, axis=0, tiled=True)
    from_audio = jnp.dot(placed, audio_full, preferred_element_type=F32)
    from_video = jnp.dot(placed, video_full, preferred_element_type=F32)
    selected = jnp.where(tags[:, 3:4] > 0, from_audio, from_video)
    return rotate(selected, tags[:, :3].T).astype(BF16)


def pack_kernel(
    frames_ref, ga_ref, gv_ref, pos_ref, dev_ref, slot_ref, count_ref, *rest, zs, part
):
    outs, flipped = rest[:zs], rest[zs]
    tok_rows, features = frames_ref.shape
    z = lax.axis_index("seq")
    c = lax.axis_index("sub")
    count = count_ref[...][None, :]
    values = frames_ref[...].astype(F32)
    mean_square = jnp.mean(values * values, axis=-1, keepdims=True)
    row = lax.broadcasted_iota(jnp.int32, (tok_rows, features), 0)
    row_gain = jnp.where(row < count, ga_ref[...][None, :], gv_ref[...][None, :])
    normed = values * lax.rsqrt(mean_square + 1e-06) * row_gain
    flipped[...] = normed.T.astype(BF16)
    lane = lax.broadcasted_iota(jnp.int32, (1, tok_rows), 1)
    pos = pos_ref[...]
    facts = [dev_ref[...][None, :], slot_ref[...][None, :], (lane < count).astype(jnp.int32)]
    for k in range(3):
        facts += [pos[k : k + 1] // DIGIT, pos[k : k + 1] % DIGIT]
    line = lax.broadcasted_iota(jnp.int32, (META, tok_rows), 0)
    meta = jnp.zeros((META, tok_rows), jnp.int32)
    for k, fact in enumerate(facts):
        meta = jnp.where(line == k, fact, meta)
    meta = meta.astype(F32).astype(BF16)
    span = features // zs
    for r in range(zs):
        start = pl.multiple_of((z ^ r) * span + c * part, 16)
        outs[r][pl.ds(0, part), :] = flipped[pl.ds(start, part), :]
        outs[r][pl.ds(part, META), :] = meta


def order_kernel(*refs, zs, xs, part, rels):
    many = (len(refs) - 4) // 2
    own_refs, twin_refs, outs = refs[:many], refs[many : 2 * many], refs[2 * many :]
    tok_rows = own_refs[0].shape[2]
    z = lax.axis_index("seq")
    x = lax.axis_index("mdl")
    c = lax.axis_index("sub")
    rows = len(rels) * tok_rows
    picks = []
    for ref in own_refs:
        for s in range(ref.shape[0]):
            head = ref[s, pl.ds(part, META), :].astype(F32).astype(jnp.int32)
            dev, slot = head[0:1], head[1:2]
            rel = (dev // xs) ^ z
            target = jnp.full_like(rel, -1)
            for i, r in enumerate(rels):
                target = jnp.where(rel == r, i * tok_rows + slot, target)
            target = jnp.where(dev % xs == x, target, -1)
            line = lax.broadcasted_iota(jnp.int32, (rows, tok_rows), 0)
            picks.append((line == target).astype(F32).astype(BF16))
    pick = jnp.concatenate(picks, axis=1)
    nt = (((1,), (1,)), ((), ()))
    got = []
    for side in (own_refs, twin_refs):
        wide = jnp.concatenate([ref[s] for ref in side for s in range(ref.shape[0])], axis=1)
        got.append(lax.dot_general(pick, wide, nt, preferred_element_type=F32))
    if rels[0] == 0:
        outs[4][...] = got[0][:tok_rows, part:]
    audio = got[0][:, part + 2 : part + 3] > 0.5
    same = x == c
    first = jnp.where(same, got[0][:, :part], got[1][:, :part])
    other = jnp.where(same, got[1][:, :part], got[0][:, :part])
    for k, values in enumerate((first, other)):
        outs[2 * k][...] = jnp.where(audio, values, 0.0).astype(BF16)
        outs[2 * k + 1][...] = jnp.where(audio, 0.0, values).astype(BF16)


def project_kernel(oa_ref, ov_ref, pa_ref, pv_ref, own_a, own_v, *refs, places):
    peers, outs = refs[: len(places)], refs[len(places) :]
    part, half = own_a.shape[0], own_a.shape[1] // 2
    tok_rows = outs[0].shape[0]
    step = 256
    done = 0
    for (flip, base), peer_ref in zip(places, peers):
        h = lax.axis_index("grp") ^ flip
        for at in range(0, peer_ref.shape[1], step):
            size = min(step, peer_ref.shape[1] - at)
            lanes = pl.ds(pl.multiple_of(h * half + base + at, 128), size)
            there = pl.ds(at, size)
            total = jnp.dot(oa_ref[...], own_a[:, lanes], preferred_element_type=F32)
            total += jnp.dot(ov_ref[...], own_v[:, lanes], preferred_element_type=F32)
            total += jnp.dot(pa_ref[...], peer_ref[:part, there], preferred_element_type=F32)
            total += jnp.dot(pv_ref[...], peer_ref[part:, there], preferred_element_type=F32)
            for i, out in enumerate(outs):
                block = total[i * tok_rows : (i + 1) * tok_rows]
                out[:, pl.ds(done + at, size)] = block.astype(out.dtype)
        done += peer_ref.shape[1]


def finish_kernel(cos_ref, sin_ref, *refs, places):
    out_ref, turned_ref, sent = refs[-3:]
    parts = len(refs[:-3]) // len(places)
    half = out_ref.shape[1] // 2
    y = lax.axis_index("grp")
    cosine = jnp.concatenate([cos_ref[...], cos_ref[...]], axis=1)
    sinus = jnp.concatenate([-sin_ref[...], sin_ref[...]], axis=1)
    copies, begin = [], 0
    for i, pieces in enumerate(places):
        chunk = refs[i * parts : (i + 1) * parts]
        at = 0
        for flip, base, size in pieces:
            for head in range(0, size, HEAD):
                lanes = pl.ds(at + head, HEAD)
                total = chunk[0][:, lanes]
                for piece in chunk[1:]:
                    total = total + piece[:, lanes].astype(F32)
                turned = total * cosine + pltpu.roll(total, HEAD // 2, 1) * sinus
                turned_ref[:, pl.ds(begin + head, HEAD)] = turned.astype(BF16)
            where = pl.ds(pl.multiple_of((y ^ flip) * half + base, HEAD), size)
            source = turned_ref.at[:, pl.ds(begin, size)]
            copies.append(
                pltpu.make_async_copy(source, out_ref.at[:, where], sent.at[len(copies)])
            )
            copies[-1].start()
            at, begin = at + size, begin + size
    for copy in copies:
        copy.wait()


def vmem(n):
    return [pl.BlockSpec(memory_space=pltpu.VMEM) for _ in range(n)]


def swap(value, axis, r):
    n = lax.axis_size(axis)
    return lax.ppermute(value, axis, [(i, i ^ r) for i in range(n)])


def halved_plan(
    frames, audio_count, pos_ids, gain_audio, gain_video, audio_proj, video_proj, dest_device, dest_slot
):
    tok_rows, features = frames.shape
    zs, xs = lax.axis_size("seq"), lax.axis_size("mdl")
    part = audio_proj.shape[0]
    width = audio_proj.shape[1]
    half = width // 2
    y = lax.axis_index("grp")

    heads = half // HEAD
    marks = [heads * at // sum(CUTS) * HEAD for at in itertools.accumulate(CUTS, initial=0)]
    cuts = [(a, b - a) for a, b in zip(marks, marks[1:])]
    row, rest = [], []
    for i, (base, size) in enumerate(cuts):
        both = [
            lax.dynamic_slice_in_dim(proj, y * half + base, size, 1)
            for proj in (audio_proj, video_proj)
        ]
        row.append(swap(jnp.concatenate(both), "mdl", 1))
        rest.append(swap(row[i], "grp", 1))

    shape = jax.ShapeDtypeStruct
    given = (frames, gain_audio, gain_video, pos_ids, dest_device, dest_slot, audio_count)
    packed = pl.pallas_call(
        functools.partial(pack_kernel, zs=zs, part=part),
        out_shape=[shape((part + META, tok_rows), BF16)] * zs,
        in_specs=vmem(len(given)),
        out_specs=vmem(zs),
        scratch_shapes=[pltpu.VMEM((features, tok_rows), BF16)],
        compiler_params=pltpu.CompilerParams(vmem_limit_bytes=GRANT),
        name="pack",
    )(*given)
    blocks = [packed[0]] + [swap(packed[r], "seq", r) for r in ARRIVAL]
    columns = [jnp.stack(blocks[:2]), jnp.stack(blocks[2:])]
    columns += [swap(v, "mdl", 1) for v in columns]
    twins = [swap(v, "sub", 1) for v in columns]

    ahead = [r for r in range(zs) if r % 2 and r > 1]
    groups = [ahead, [r for r in range(zs) if r not in ahead]]
    ordered = []
    for rels in groups:
        extra = [shape((tok_rows, META), F32)] if rels[0] == 0 else []
        call = pl.pallas_call(
            functools.partial(order_kernel, zs=zs, xs=xs, part=part, rels=rels),
            out_shape=[shape((len(rels) * tok_rows, part), BF16)] * 4 + extra,
            in_specs=vmem(2 * len(columns)),
            out_specs=vmem(4 + len(extra)),
            compiler_params=pltpu.CompilerParams(vmem_limit_bytes=GRANT),
            name="order",
        )
        ordered.append(call(*columns, *twins))
    meta = ordered[1][4]

    def project(pieces):
        peers = [(rest if flip else row)[i] for i, flip in pieces]
        across = sum(peer.shape[1] for peer in peers)
        at = tuple((flip, cuts[i][0]) for i, flip in pieces)
        blocks = {}
        for g, rels in enumerate(groups):
            call = pl.pallas_call(
                functools.partial(project_kernel, places=at),
                out_shape=[shape((tok_rows, across), BF16 if r % 2 else F32) for r in rels],
                in_specs=vmem(6 + len(peers)),
                out_specs=vmem(len(rels)),
                compiler_params=pltpu.CompilerParams(vmem_limit_bytes=GRANT),
                name="project",
            )
            made = call(*ordered[g][:4], audio_proj, video_proj, *peers)
            blocks.update(zip(rels, made))
        return blocks

    chunks, places = [], []
    for pieces in CHUNKS:
        blocks = project(pieces)
        step, arrived = 1, [blocks[0]]
        while step < zs:
            later = [r for r in blocks if r % (2 * step) == step and r != step]
            moved = {r: swap(blocks[r].astype(BF16), "seq", step) for r in later}
            arrived.append(swap(blocks[step].astype(BF16), "seq", step))
            for r in later:
                blocks[r ^ step] = blocks[r ^ step].astype(F32) + moved[r].astype(F32)
            step *= 2
        chunks += arrived
        places.append(tuple((flip, *cuts[i]) for i, flip in pieces))

    whole = [meta[:, 3 + 2 * k] * DIGIT + meta[:, 4 + 2 * k] for k in range(3)]
    angles = angles_of(whole)
    return pl.pallas_call(
        functools.partial(finish_kernel, places=places),
        out_shape=shape((tok_rows, width), BF16),
        in_specs=vmem(2 + len(chunks)),
        out_specs=pl.BlockSpec(memory_space=pltpu.HBM),
        scratch_shapes=[
            pltpu.VMEM((tok_rows, width), BF16),
            pltpu.SemaphoreType.DMA((sum(len(place) for place in places),)),
        ],
        compiler_params=pltpu.CompilerParams(vmem_limit_bytes=GRANT),
        name="finish",
    )(jnp.cos(angles), jnp.sin(angles), *chunks)


def fits(mesh, features, width):
    size = dict(mesh.shape)
    zs = size["seq"]
    rows = features // (zs * size["mdl"])
    pairs = all(size[axis] == 2 for axis in ("grp", "mdl", "sub"))
    return pairs and zs == 1 + len(ARRIVAL) and rows % 16 == 0 and width % 256 == 0


def solution(mesh):
    def on_device(*args):
        ok = fits(mesh, args[0].shape[1], args[5].shape[1])
        return (halved_plan if ok else gathered_plan)(*args)

    in_specs = (
        P(("grp", "seq", "mdl"), None),
        P(("grp", "seq", "mdl")),
        P(None, ("grp", "seq", "mdl")),
        P(),
        P(),
        P(("seq", "mdl"), "sub"),
        P(("seq", "mdl"), "sub"),
        P(("grp", "seq", "mdl")),
        P(("grp", "seq", "mdl")),
    )
    out_specs = P(("grp", "seq", "mdl"), "sub")
    return jax.shard_map(
        on_device, mesh=mesh, in_specs=in_specs, out_specs=out_specs, check_vma=False
    )
```
